32 devices in a mesh: dp: 16 (over z, y, x), mp: 2 (over core).
Axes of the slice: x: 2, y: 2, z: 4, core: 2. Of those that a mesh axis runs over, the one named last changes fastest.
Arguments:
- q_new: bfloat16 [32, 8, 256], P('dp', 'mp'), may hold values from -6 to 6
- k_new: bfloat16 [32, 8, 256], P('dp', 'mp'), may hold values from -6 to 6
- v_new: bfloat16 [32, 8, 256], P('dp', 'mp'), may hold values from -6 to 6
- k_cache: bfloat16 [32, 8, 1024, 256], P('dp', 'mp'), may hold values from -6 to 6
- v_cache: bfloat16 [32, 8, 1024, 256], P('dp', 'mp'), may hold values from -6 to 6
- lengths: int32 [32], P('dp'), may hold values from 1 to 1024
- memory: float32 [32, 8, 256, 256], P('dp', 'mp'), may hold values from -6 to 6
- norm_z: float32 [32, 8, 256], P('dp', 'mp'), may hold values from 0.01 to 0.1
- beta: float32 [8], P('mp'), may hold values from -2 to 2
- out_weight: bfloat16 [2048, 2048], P(None, 'mp'), may hold values from -0.125 to 0.125
- residual_in: bfloat16 [32, 2048], P('dp', 'mp'), may hold values from -45 to 45
- final_gain: float32 [2048], replicated, may hold values from 0.5 to 1.5
- embedding: bfloat16 [8192, 2048], P(('dp', 'mp')), may hold values from -0.9943689 to 0.9943689
Outputs:
- hidden_out: bfloat16 [32, 2048], P('dp', 'mp')
- log_probs: float32 [32, 8192], P(None, ('dp', 'mp'))
The draws below stay inside these ranges and needn't reach their ends.
All inputs are finite; a program needn't handle non-finite values.
Results may differ from the reference program's by a relative error of at most 0.0033.
Values may be sent and summed in bfloat16 or wider, within the bound.
A program may use at most 64 MiB of HBM per device.

```python
import math
import jax
import jax.numpy as jnp
from jax import lax

D = 2048
HEADS = 8
HD = 256
CACHE = 1024
STREAMS = 32
VOCAB = 8192


def draw_residual_in(key, part):
    first, second, third = jax.random.split(jax.random.fold_in(key, 11), 3)
    row_scale = jnp.exp(jax.random.uniform(first, (STREAMS, 1), jnp.float32) * jnp.log(10.0))
    column_rise = jnp.log(3.0) * jnp.arange(D, dtype=jnp.float32) / D
    column_scale = jnp.exp(column_rise[None, :] + jax.random.uniform(second, (1, D), jnp.float32) * jnp.log(3.3))
    base = jax.random.normal(third, (STREAMS, D), jnp.float32)
    base = jnp.clip(base, -4.0, 4.0)
    return (0.1 * base * row_scale * column_scale).astype(jnp.bfloat16)


def draw_embedding(key, part):
    first, second = jax.random.split(jax.random.fold_in(key, 23), 2)
    row_rise = jnp.log(3.0) * jnp.arange(VOCAB, dtype=jnp.float32) / VOCAB
    row_scale = jnp.exp(row_rise[:, None] + jax.random.uniform(first, (VOCAB, 1), jnp.float32) * jnp.log(3.3))
    base = jax.random.normal(second, (VOCAB, D), jnp.float32)
    base = jnp.clip(base, -4.0, 4.0)
    return (base * row_scale / jnp.sqrt(jnp.float32(D))).astype(jnp.bfloat16)


def place_ends(result, own_key, low, largest):
    longest = result.shape.index(max(result.shape))
    spots = []
    for shift in (0, 1):
        where = [jax.random.randint(jax.random.fold_in(own_key, axis), (), 0, length) for axis, length in enumerate(result.shape)]
        where[longest] = (where[longest] + shift) % result.shape[longest]
        spots.append(tuple(where))
    return result.at[spots[0]].set(low).at[spots[1]].set(largest)


def block_levels(rng, dims, shards, low, high):
    gain, own = 1.0, jax.random.fold_in(rng, 6)
    for dim, parts in shards:
        heights = jnp.exp(jax.random.uniform(jax.random.fold_in(own, dim), (parts,), jnp.float32, low / len(shards), high / len(shards)))
        gain = gain * jnp.repeat(heights, dims[dim] // parts).reshape([-1 if axis == dim else 1 for axis in range(len(dims))])
    return gain


def scatter_about(key, dims, spread, reach, shards=(), kind=jnp.bfloat16):
    level = block_levels(key, dims, shards, -0.22, 0.18) if shards else 1.0
    array = jax.random.normal(key, dims, jnp.float32) * spread * level
    return jnp.minimum(jnp.maximum(array, -reach), reach).astype(kind)


def setup_inputs(seed: int = 0) -> dict:
    key_list = jax.random.split(jax.random.key(seed), 14)
    q_new = scatter_about(key_list[0], (STREAMS, HEADS, HD), 1.0, 6.0, ((0, 16), (1, 2)))
    k_new = scatter_about(key_list[1], (STREAMS, HEADS, HD), 1.0, 6.0, ((0, 16), (1, 2)))
    v_new = scatter_about(key_list[2], (STREAMS, HEADS, HD), 1.0, 6.0, ((0, 16), (1, 2)))
    k_cache = scatter_about(key_list[3], (STREAMS, HEADS, CACHE, HD), 1.0, 6.0, ((0, 16), (1, 2)))
    v_cache = scatter_about(key_list[4], (STREAMS, HEADS, CACHE, HD), 1.0, 6.0, ((0, 16), (1, 2)))
    lengths = place_ends(jax.random.randint(key_list[5], (STREAMS,), 1, CACHE + 1), jax.random.fold_in(key_list[5], 1), 1, CACHE).astype(jnp.int32)
    memory = scatter_about(key_list[6], (STREAMS, HEADS, HD, HD), 1.0, 6.0, ((0, 16), (1, 2)), jnp.float32)
    norm_z = jnp.clip(jnp.exp(math.log(0.1) - 2.3025851 * jax.random.uniform(key_list[7], (STREAMS, HEADS, HD), jnp.float32) ** block_levels(key_list[7], (STREAMS, HEADS, HD), ((0, 16), (1, 2)), -0.2, 0.2)), 0.01, 0.1)
    beta = jnp.clip(jax.random.uniform(key_list[8], (HEADS,), jnp.float32, -2.0, 2.0) * block_levels(key_list[8], (HEADS,), ((0, 2),), -0.4, 0.0), -2.0, 2.0)
    out_weight = scatter_about(key_list[9], (HEADS * HD, D), (HEADS * HD) ** -0.5, 0.125, ((1, 2),))
    residual_in = draw_residual_in(jax.random.fold_in(key_list[13], 71), 0)
    final_gain = jnp.clip(1.0 + 0.1 * jax.random.normal(key_list[11], (D,), jnp.float32), 0.5, 1.5)
    embedding = draw_embedding(jax.random.fold_in(key_list[13], 71), 0)
    return dict(q_new=q_new, k_new=k_new, v_new=v_new, k_cache=k_cache, v_cache=v_cache, lengths=lengths, memory=memory, norm_z=norm_z, beta=beta, out_weight=out_weight, residual_in=residual_in, final_gain=final_gain, embedding=embedding)


epsilon = 1e-06

def one_stream(packed):
    query, key_now, value_now, keys, values, live_count, memory_matrix, norm_vec = packed
    floating = jnp.float32
    scaling = 1.0 / math.sqrt(HD)
    scores = jnp.einsum('hd,hld->hl', query.astype(floating), keys.astype(floating))
    scores = 50.0 * jnp.tanh(scores * scaling / 50.0)
    own_score = 50.0 * jnp.tanh(lax.optimization_barrier(jnp.sum(query.astype(floating) * key_now.astype(floating), axis=-1)) * scaling / 50.0)
    live = jnp.arange(CACHE, dtype=jnp.int32)[None, :] < live_count
    weights = jnp.where(live, jnp.exp(scores), 0.0)
    self_token_weight = jnp.exp(own_score)
    summed = lax.optimization_barrier(jnp.sum(weights, axis=-1)) + self_token_weight
    weights_bf = weights.astype(jnp.bfloat16).astype(floating)
    own_bf = self_token_weight.astype(jnp.bfloat16).astype(floating)
    local = jnp.einsum('hl,hld->hd', weights_bf, values.astype(floating)) + own_bf[:, None] * value_now.astype(floating)
    local = local / summed[:, None]
    raised_features = jax.nn.elu(query.astype(floating)) + 1.0
    memory_retrieval = jnp.einsum('ad,adx->ax', raised_features, memory_matrix, precision=lax.Precision.HIGHEST)
    memory_retrieval = memory_retrieval / lax.optimization_barrier(jnp.sum(raised_features * norm_vec, axis=-1))[:, None]
    return (local, memory_retrieval)

def reference(q_new, k_new, v_new, k_cache, v_cache, lengths, memory, norm_z, beta, out_weight, residual_in, final_gain, embedding):
    floating = jnp.float32
    local, memory_retrieval = lax.map(one_stream, (q_new, k_new, v_new, k_cache, v_cache, lengths, memory, norm_z))
    gate = jax.nn.sigmoid(beta)[None, :, None]
    head_out = (gate * memory_retrieval + (1.0 - gate) * local).astype(jnp.bfloat16).reshape(STREAMS, HEADS * HD)
    hidden_out = (residual_in.astype(floating) + jnp.dot(head_out, out_weight, preferred_element_type=floating)).astype(jnp.bfloat16)
    hidden_f = hidden_out.astype(floating)
    mean_sq = lax.optimization_barrier(jnp.mean(hidden_f * hidden_f, axis=-1, keepdims=True))
    normed = (hidden_f * lax.rsqrt(mean_sq + epsilon) * final_gain[None, :]).astype(jnp.bfloat16)
    logits = 30.0 * jnp.tanh(jnp.dot(normed, embedding.T, preferred_element_type=floating) / 30.0)
    log_total = jnp.log(lax.optimization_barrier(jnp.sum(jnp.exp(logits), axis=-1, keepdims=True)))
    return (hidden_out, logits - log_total)
```

```python
import functools
import math

import jax
import jax.numpy as jnp
from jax import lax
from jax.experimental import pallas as pl
from jax.experimental.pallas import tpu as pltpu
from jax.sharding import PartitionSpec as P

MESH = pl.DeviceIdType.MESH
F32 = jnp.float32
BF16 = jnp.bfloat16
LANES = 128
epsilon = 1e-06

NT = (((1,), (1,)), ((), ()))


def up(value, step):
    return -(-value // step) * step


def kernel(
    DP, MP, B, H, HD, L, FW, CP,
    lengths_ref, beta_ref, q_hbm, kn_hbm, vn_hbm, k_hbm, v_hbm, mem_hbm, nz_hbm, w_hbm, res_hbm, gain_hbm, e_hbm,
    hid_ref, out_ref,
    q_in, kn_in, vn_in, nz_in, res, gain, k_vm, v_vm, m_vm, w_vm, e_vm,
    flat, heads, tile, gath, gf, sums,
    small_sem, k_sem, v_sem, m_sem, w_sem, e_sem,
    h_send, h_recv, g_send, g_recv, s_send, s_recv,
):
    dp, mp = lax.axis_index("dp"), lax.axis_index("mp")
    N = DP * MP
    me = dp * MP + mp
    slot = mp * DP + dp
    pairs = [(b, h) for b in range(B) for h in range(H)]
    PP = flat.shape[1]
    C = FW // LANES
    D = MP * FW
    S = DP * B
    HW = H * HD

    small = [
        pltpu.make_async_copy(src, dst, small_sem.at[i])
        for i, (src, dst) in enumerate(
            [(q_hbm, q_in), (kn_hbm, kn_in), (nz_hbm, nz_in), (vn_hbm, vn_in), (res_hbm, res), (gain_hbm, gain)]
        )
    ]
    k_copy = [pltpu.make_async_copy(k_hbm.at[b, h], k_vm.at[i], k_sem.at[i]) for i, (b, h) in enumerate(pairs)]
    v_copy = [pltpu.make_async_copy(v_hbm.at[b, h], v_vm.at[i], v_sem.at[i]) for i, (b, h) in enumerate(pairs)]
    m_copy = [pltpu.make_async_copy(mem_hbm.at[b, h], m_vm.at[i], m_sem.at[i]) for i, (b, h) in enumerate(pairs)]
    w_copy = []
    for i in range(MP):
        rows = pl.ds(pl.multiple_of(lax.rem(mp + i, MP) * HW, HW), HW)
        w_copy.append(pltpu.make_async_copy(w_hbm.at[rows], w_vm.at[rows], w_sem.at[i]))
    e_copy = pltpu.make_async_copy(e_hbm, e_vm, e_sem)
    for copy in small[:4] + k_copy + m_copy + v_copy + small[4:] + w_copy + [e_copy]:
        copy.start()

    barrier = pltpu.get_barrier_semaphore()

    @pl.loop(1, N)
    def _(i):
        p = lax.rem(me + i, N)
        pl.semaphore_signal(barrier, inc=1, device_id=(p // MP, lax.rem(p, MP)), device_id_type=MESH)

    if PP != len(pairs):
        flat[...] = jnp.zeros_like(flat)
    row = lax.broadcasted_iota(jnp.int32, (PP, 1), 0)
    for i, src in enumerate([q_in, kn_in, nz_in, vn_in]):
        small[i].wait()
        for b in range(B):
            flat[i, b * H : (b + 1) * H, :] = src[b].astype(F32)
    q, kn, nz, vn = flat[0], flat[1], flat[2], flat[3]
    qb = q.astype(BF16)
    scaling = 1.0 / math.sqrt(HD)

    own = jnp.exp(50.0 * jnp.tanh(jnp.sum(q * kn, axis=1, keepdims=True) * scaling / 50.0))
    sq = jnp.where(q > 0.0, q, jnp.exp(jnp.minimum(q, 0.0)) - 1.0) + 1.0
    denominator = jnp.sum(sq * nz, axis=1, keepdims=True)
    sq_hi = sq.astype(BF16)
    sq_lo = (sq - sq_hi.astype(F32)).astype(BF16)
    sq_both = jnp.concatenate([sq_hi.astype(F32), sq_lo.astype(F32)], axis=0).astype(BF16)

    scores = jnp.zeros((PP, L), F32)
    for i in range(len(pairs)):
        k_copy[i].wait()
        part = lax.dot_general(qb, k_vm[i], NT, preferred_element_type=F32)
        scores = jnp.where(row == i, part, scores)
    live_count = jnp.zeros((PP, 1), jnp.int32)
    gate = jnp.zeros((PP, 1), F32)
    for i, (b, h) in enumerate(pairs):
        live_count = jnp.where(row == i, lengths_ref[b], live_count)
        gate = jnp.where(row == i, beta_ref[h], gate)
    gate = 1.0 / (1.0 + jnp.exp(-gate))
    weights = jnp.exp(50.0 * jnp.tanh(scores * scaling / 50.0))
    live = lax.broadcasted_iota(jnp.int32, (PP, L), 1) < live_count
    weights = jnp.where(live, weights, 0.0)
    total = jnp.sum(weights, axis=1, keepdims=True) + own
    wb = weights.astype(BF16)

    readout = jnp.zeros((PP, HD), F32)
    for i in range(len(pairs)):
        m_copy[i].wait()
        m = m_vm[i]
        m_hi = m.astype(BF16)
        m_lo = (m - m_hi.astype(F32)).astype(BF16)
        first = jnp.dot(sq_both, m_hi, preferred_element_type=F32)
        second = jnp.dot(sq_hi, m_lo, preferred_element_type=F32)
        readout = jnp.where(row == i, first[:PP] + first[PP:] + second, readout)
    readout = readout / denominator

    local = jnp.zeros((PP, HD), F32)
    for i in range(len(pairs)):
        v_copy[i].wait()
        part = jnp.dot(wb, v_vm[i], preferred_element_type=F32)
        local = jnp.where(row == i, part, local)
    local = (local + own.astype(BF16).astype(F32) * vn) / total
    head_out = gate * readout + (1.0 - gate) * local
    heads[mp] = head_out.astype(BF16)

    pl.semaphore_wait(barrier, N - 1)

    def head_send(i):
        m = lax.rem(mp + i, MP)
        return pltpu.make_async_remote_copy(
            src_ref=heads.at[mp], dst_ref=heads.at[mp],
            send_sem=h_send.at[i], recv_sem=h_recv.at[mp],
            device_id=(dp, m), device_id_type=MESH,
        )

    for i in range(1, MP):
        head_send(i).start()

    small[4].wait()
    small[5].wait()
    turn = lax.rem(row, H)
    acc = None
    for i in range(MP):
        m = lax.rem(mp + i, MP)
        w_copy[i].wait()
        if i:
            pltpu.make_async_copy(heads.at[m], heads.at[m], h_recv.at[m]).wait()
        ho = heads[m].astype(F32)
        lhs = jnp.concatenate([jnp.where(turn == h, ho, 0.0) for h in range(H)], axis=1).astype(BF16)
        part = jnp.dot(lhs, w_vm[pl.ds(pl.multiple_of(m * HW, HW), HW), :], preferred_element_type=F32)
        acc = part if acc is None else acc + part

    res_f = res[...].astype(F32)
    if CP != C:
        tile[...] = jnp.zeros_like(tile)
    hidden = []
    for b in range(B):
        mine = jnp.where((row >= b * H) & (row < (b + 1) * H), acc, 0.0)
        h_b = res_f[b : b + 1] + jnp.sum(mine, axis=0, keepdims=True)
        hidden.append(h_b)
        for c in range(C):
            tile[b * CP + c : b * CP + c + 1, :] = h_b[:, c * LANES : (c + 1) * LANES]
    gath[slot] = tile[...].astype(BF16)

    @pl.loop(1, N)
    def _(i):
        p = lax.rem(me + i, N)
        pltpu.make_async_remote_copy(
            src_ref=gath.at[slot], dst_ref=gath.at[slot], send_sem=g_send, recv_sem=g_recv,
            device_id=(p // MP, lax.rem(p, MP)), device_id_type=MESH,
        ).start()

    hid_ref[...] = jnp.concatenate(hidden, axis=0).astype(BF16)
    e_copy.wait()
    others = gath.at[pl.ds(0, N - 1)]
    pltpu.make_async_copy(others, others, g_recv).wait()

    RP = B * CP
    gf[...] = gath[...].astype(F32).reshape(MP, DP * RP, LANES)
    columns = [gf[m, pl.ds(c, S, stride=CP), :] for m in range(MP) for c in range(C)]
    square = functools.reduce(jnp.add, [x * x for x in columns])
    scale = lax.rsqrt(jnp.sum(square, axis=1, keepdims=True) / D + epsilon)
    normed = [(x * scale * gain[:, j * LANES : (j + 1) * LANES]) for j, x in enumerate(columns)]
    normed = jnp.concatenate(normed, axis=1).astype(BF16)
    logits = lax.dot_general(normed, e_vm[...], NT, preferred_element_type=F32)
    logits = 30.0 * jnp.tanh(logits / 30.0)
    mine = jnp.sum(jnp.exp(logits), axis=1, keepdims=True)
    wide = sums.shape[2]
    diagonal = lax.broadcasted_iota(jnp.int32, (S, wide), 0) == lax.broadcasted_iota(jnp.int32, (S, wide), 1)
    sums[me] = jnp.sum(jnp.where(diagonal, mine, 0.0), axis=0, keepdims=True)

    @pl.loop(1, N)
    def _(i):
        p = lax.rem(me + i, N)
        pltpu.make_async_remote_copy(
            src_ref=sums.at[me], dst_ref=sums.at[me], send_sem=s_send, recv_sem=s_recv,
            device_id=(p // MP, lax.rem(p, MP)), device_id_type=MESH,
        ).start()

    others_s = sums.at[pl.ds(0, N - 1)]
    pltpu.make_async_copy(others_s, others_s, s_recv).wait()
    everything = jnp.sum(sums[...], axis=0)
    log_total = jnp.log(jnp.sum(jnp.where(diagonal, everything, 0.0), axis=1, keepdims=True))
    out_ref[...] = logits - log_total

    for i in range(1, MP):
        head_send(i).wait_send()
    pltpu.make_async_copy(others, others, g_send).wait()
    pltpu.make_async_copy(others_s, others_s, s_send).wait()


def solution(mesh):
    DP, MP = mesh.shape["dp"], mesh.shape["mp"]
    N = DP * MP

    def body(q_new, k_new, v_new, k_cache, v_cache, lengths, memory, norm_z, beta, out_weight, residual_in, final_gain, embedding):
        B, H, L, HD = k_cache.shape
        FW = out_weight.shape[1]
        V, D = embedding.shape
        C = FW // LANES
        CP = up(C, 16 // math.gcd(B, 16))
        pairs, PP = B * H, up(B * H, 8)
        S = DP * B
        dma = pltpu.SemaphoreType.DMA
        anywhere = pl.BlockSpec(memory_space=pl.ANY)
        vmem = pl.BlockSpec(memory_space=pltpu.VMEM)
        smem = pl.BlockSpec(memory_space=pltpu.SMEM)
        return pl.pallas_call(
            functools.partial(kernel, DP, MP, B, H, HD, L, FW, CP),
            out_shape=(jax.ShapeDtypeStruct((B, FW), BF16), jax.ShapeDtypeStruct((S, V), F32)),
            in_specs=[smem] * 2 + [anywhere] * 11,
            out_specs=(vmem, vmem),
            scratch_shapes=[
                pltpu.VMEM((B, H, HD), BF16),
                pltpu.VMEM((B, H, HD), BF16),
                pltpu.VMEM((B, H, HD), BF16),
                pltpu.VMEM((B, H, HD), F32),
                pltpu.VMEM((B, FW), BF16),
                pltpu.VMEM((1, D), F32),
                pltpu.VMEM((pairs, L, HD), BF16),
                pltpu.VMEM((pairs, L, HD), BF16),
                pltpu.VMEM((pairs, HD, HD), F32),
                pltpu.VMEM(out_weight.shape, BF16),
                pltpu.VMEM((V, D), BF16),
                pltpu.VMEM((4, PP, HD), F32),
                pltpu.VMEM((MP, PP, HD), BF16),
                pltpu.VMEM((B * CP, LANES), F32),
                pltpu.VMEM((N, B * CP, LANES), BF16),
                pltpu.VMEM((MP, DP * B * CP, LANES), F32),
                pltpu.VMEM((N, 1, up(S, LANES)), F32),
                dma((6,)),
                dma((pairs,)),
                dma((pairs,)),
                dma((pairs,)),
                dma((MP,)),
                dma,
                dma((MP,)),
                dma((MP,)),
                dma,
                dma,
                dma,
                dma,
            ],
            compiler_params=pltpu.CompilerParams(collective_id=0, has_side_effects=True),
            name="decode_step",
        )(
            lengths, beta, q_new, k_new, v_new, k_cache, v_cache, memory, norm_z, out_weight, residual_in,
            final_gain.reshape(1, D), embedding,
        )

    in_specs = (
        P("dp", "mp", None),
        P("dp", "mp", None),
        P("dp", "mp", None),
        P("dp", "mp", None, None),
        P("dp", "mp", None, None),
        P("dp"),
        P("dp", "mp", None, None),
        P("dp", "mp", None),
        P("mp"),
        P(None, "mp"),
        P("dp", "mp"),
        P(),
        P(("dp", "mp"), None),
    )
    out_specs = (P("dp", "mp"), P(None, ("dp", "mp")))
    return jax.shard_map(body, mesh=mesh, in_specs=in_specs, out_specs=out_specs, check_vma=False)
```

```python
import functools
import math

import jax
import jax.numpy as jnp
from jax import lax
from jax.experimental import pallas as pl
from jax.experimental.pallas import tpu as pltpu
from jax.sharding import PartitionSpec as P

MESH = pl.DeviceIdType.MESH
F32 = jnp.float32
BF16 = jnp.bfloat16
LANES = 128
epsilon = 1e-06

NT = (((1,), (1,)), ((), ()))


def up(value, step):
    return -(-value // step) * step


def kernel(
    DP, MP, B, H, HD, L, FW, CP,
    lengths_ref, beta_ref, q_hbm, kn_hbm, vn_hbm, k_hbm, v_hbm, mem_hbm, nz_hbm, w_hbm, res_hbm, gain_hbm, e_hbm,
    hid_ref, out_ref,
    q_in, kn_in, vn_in, nz_in, res, gain, k_vm, v_vm, m_vm, w_vm, e_vm,
    len_sm, beta_sm, flat, heads, tile, gath, gf, sums, parts,
    small_sem, k_sem, v_sem, m_sem, w_sem, e_sem,
    h_send, h_recv, g_send, g_recv, s_send, s_recv, p_send, p_recv, t_send, t_recv,
):
    dp, mp = lax.axis_index("dp"), lax.axis_index("mp")
    slot = mp * DP + dp
    pairs = [(b, h) for b in range(B) for h in range(H)]
    PP = flat.shape[1]
    C = FW // LANES
    D = MP * FW
    S = DP * B
    HW = H * HD

    barrier = pltpu.get_barrier_semaphore()

    @pl.loop(1, DP)
    def _(i):
        pl.semaphore_signal(barrier, inc=1, device_id=(lax.rem(dp + i, DP), mp), device_id_type=MESH)

    for i in range(1, MP):
        pl.semaphore_signal(barrier, inc=1, device_id=(dp, lax.rem(mp + i, MP)), device_id_type=MESH)

    small = [
        pltpu.make_async_copy(src, dst, small_sem.at[i])
        for i, (src, dst) in enumerate(
            [(q_hbm, q_in), (kn_hbm, kn_in), (nz_hbm, nz_in), (vn_hbm, vn_in), (res_hbm, res), (gain_hbm, gain), (lengths_ref, len_sm), (beta_ref, beta_sm)]
        )
    ]
    k_copy = [pltpu.make_async_copy(k_hbm.at[b, h], k_vm.at[i], k_sem.at[i]) for i, (b, h) in enumerate(pairs)]
    v_copy = [pltpu.make_async_copy(v_hbm.at[b, h], v_vm.at[i], v_sem.at[i]) for i, (b, h) in enumerate(pairs)]
    m_copy = [pltpu.make_async_copy(mem_hbm.at[b, h], m_vm.at[i], m_sem.at[i]) for i, (b, h) in enumerate(pairs)]
    w_copy = []
    for i in range(MP):
        rows = pl.ds(pl.multiple_of(lax.rem(mp + i, MP) * HW, HW), HW)
        w_copy.append(pltpu.make_async_copy(w_hbm.at[rows], w_vm.at[rows], w_sem.at[i]))
    e_copy = pltpu.make_async_copy(e_hbm, e_vm, e_sem)
    for copy in small[:4] + small[6:] + k_copy + m_copy + v_copy + small[4:6] + w_copy + [e_copy]:
        copy.start()

    if PP != len(pairs):
        flat[...] = jnp.zeros_like(flat)
    row = lax.broadcasted_iota(jnp.int32, (PP, 1), 0)
    for i, src in enumerate([q_in, kn_in, nz_in, vn_in]):
        small[i].wait()
        for b in range(B):
            flat[i, b * H : (b + 1) * H, :] = src[b].astype(F32)
    q, kn, nz, vn = flat[0], flat[1], flat[2], flat[3]
    qb = q.astype(BF16)
    scaling = 1.0 / math.sqrt(HD)

    own = jnp.exp(50.0 * jnp.tanh(jnp.sum(q * kn, axis=1, keepdims=True) * scaling / 50.0))
    sq = jnp.where(q > 0.0, q, jnp.exp(jnp.minimum(q, 0.0)) - 1.0) + 1.0
    denominator = jnp.sum(sq * nz, axis=1, keepdims=True)
    sq_hi = sq.astype(BF16)
    sq_lo = (sq - sq_hi.astype(F32)).astype(BF16)
    sq_both = jnp.concatenate([sq_hi.astype(F32), sq_lo.astype(F32)], axis=0).astype(BF16)

    scores = jnp.zeros((PP, L), F32)
    for i in range(len(pairs)):
        k_copy[i].wait()
        part = lax.dot_general(qb, k_vm[i], NT, preferred_element_type=F32)
        scores = jnp.where(row == i, part, scores)
    small[6].wait()
    small[7].wait()
    live_count = jnp.zeros((PP, 1), jnp.int32)
    gate = jnp.zeros((PP, 1), F32)
    for i, (b, h) in enumerate(pairs):
        live_count = jnp.where(row == i, len_sm[b], live_count)
        gate = jnp.where(row == i, beta_sm[h], gate)
    gate = 1.0 / (1.0 + jnp.exp(-gate))
    weights = jnp.exp(50.0 * jnp.tanh(scores * scaling / 50.0))
    live = lax.broadcasted_iota(jnp.int32, (PP, L), 1) < live_count
    weights = jnp.where(live, weights, 0.0)
    total = jnp.sum(weights, axis=1, keepdims=True) + own
    wb = weights.astype(BF16)

    readout = jnp.zeros((PP, HD), F32)
    for i in range(len(pairs)):
        m_copy[i].wait()
        m = m_vm[i]
        m_hi = m.astype(BF16)
        m_lo = (m - m_hi.astype(F32)).astype(BF16)
        first = jnp.dot(sq_both, m_hi, preferred_element_type=F32)
        second = jnp.dot(sq_hi, m_lo, preferred_element_type=F32)
        readout = jnp.where(row == i, first[:PP] + first[PP:] + second, readout)
    readout = readout / denominator

    local = jnp.zeros((PP, HD), F32)
    for i in range(len(pairs)):
        v_copy[i].wait()
        part = jnp.dot(wb, v_vm[i], preferred_element_type=F32)
        local = jnp.where(row == i, part, local)
    local = (local + own.astype(BF16).astype(F32) * vn) / total
    head_out = gate * readout + (1.0 - gate) * local
    heads[mp] = head_out.astype(BF16)

    pl.semaphore_wait(barrier, DP - 1 + MP - 1)

    def head_send(i):
        m = lax.rem(mp + i, MP)
        return pltpu.make_async_remote_copy(
            src_ref=heads.at[mp], dst_ref=heads.at[mp],
            send_sem=h_send.at[i], recv_sem=h_recv.at[mp],
            device_id=(dp, m), device_id_type=MESH,
        )

    for i in range(1, MP):
        head_send(i).start()

    small[4].wait()
    small[5].wait()
    turn = lax.rem(row, H)
    acc = None
    for i in range(MP):
        m = lax.rem(mp + i, MP)
        w_copy[i].wait()
        if i:
            pltpu.make_async_copy(heads.at[m], heads.at[m], h_recv.at[m]).wait()
        ho = heads[m].astype(F32)
        lhs = jnp.concatenate([jnp.where(turn == h, ho, 0.0) for h in range(H)], axis=1).astype(BF16)
        part = jnp.dot(lhs, w_vm[pl.ds(pl.multiple_of(m * HW, HW), HW), :], preferred_element_type=F32)
        acc = part if acc is None else acc + part

    res_f = res[...].astype(F32)
    if CP != C:
        tile[...] = jnp.zeros_like(tile)
    hidden = []
    for b in range(B):
        mine = jnp.where((row >= b * H) & (row < (b + 1) * H), acc, 0.0)
        h_b = res_f[b : b + 1] + jnp.sum(mine, axis=0, keepdims=True)
        hidden.append(h_b)
        for c in range(C):
            tile[b * CP + c : b * CP + c + 1, :] = h_b[:, c * LANES : (c + 1) * LANES]
    gath[slot] = tile[...].astype(BF16)

    @pl.loop(1, DP)
    def _(i):
        pltpu.make_async_remote_copy(
            src_ref=gath.at[slot], dst_ref=gath.at[slot], send_sem=g_send, recv_sem=g_recv,
            device_id=(lax.rem(dp + i, DP), mp), device_id_type=MESH,
        ).start()

    hid_ref[...] = jnp.concatenate(hidden, axis=0).astype(BF16)
    e_copy.wait()
    others = gath.at[pl.ds(0, DP - 1)]
    pltpu.make_async_copy(others, others, g_recv).wait()

    def block(m):
        return gath.at[pl.ds(pl.multiple_of(m * DP, DP), DP)]

    def relay(i):
        return pltpu.make_async_remote_copy(
            src_ref=block(mp), dst_ref=block(mp), send_sem=p_send.at[i], recv_sem=p_recv.at[mp],
            device_id=(dp, lax.rem(mp + i, MP)), device_id_type=MESH,
        )

    for i in range(1, MP):
        relay(i).start()
    for i in range(1, MP):
        m = lax.rem(mp + i, MP)
        pltpu.make_async_copy(block(m), block(m), p_recv.at[m]).wait()

    RP = B * CP
    gf[...] = gath[...].astype(F32).reshape(MP, DP * RP, LANES)
    columns = [gf[m, pl.ds(c, S, stride=CP), :] for m in range(MP) for c in range(C)]
    square = functools.reduce(jnp.add, [x * x for x in columns])
    scale = lax.rsqrt(jnp.sum(square, axis=1, keepdims=True) / D + epsilon)
    normed = [(x * scale * gain[:, j * LANES : (j + 1) * LANES]) for j, x in enumerate(columns)]
    normed = jnp.concatenate(normed, axis=1).astype(BF16)
    logits = lax.dot_general(normed, e_vm[...], NT, preferred_element_type=F32)
    logits = 30.0 * jnp.tanh(logits / 30.0)
    mine = jnp.sum(jnp.exp(logits), axis=1, keepdims=True)
    wide = sums.shape[2]
    diagonal = lax.broadcasted_iota(jnp.int32, (S, wide), 0) == lax.broadcasted_iota(jnp.int32, (S, wide), 1)
    sums[slot] = jnp.sum(jnp.where(diagonal, mine, 0.0), axis=0, keepdims=True)

    def sum_send(i, m):
        return pltpu.make_async_remote_copy(
            src_ref=sums.at[slot], dst_ref=sums.at[slot], send_sem=s_send, recv_sem=s_recv,
            device_id=(lax.rem(dp + i, DP), m), device_id_type=MESH,
        )

    @pl.loop(1, DP)
    def _(i):
        for j in range(MP):
            sum_send(i, lax.rem(mp + j, MP)).start()

    for j in range(1, MP):
        sum_send(0, lax.rem(mp + j, MP)).start()

    others_s = sums.at[pl.ds(0, DP * MP - 1)]
    pltpu.make_async_copy(others_s, others_s, s_recv).wait()
    everything = jnp.sum(sums[...], axis=0)
    log_total = jnp.log(jnp.sum(jnp.where(diagonal, everything, 0.0), axis=1, keepdims=True))
    out_ref[...] = logits - log_total

    for i in range(1, MP):
        head_send(i).wait_send()
        relay(i).wait_send()
    pltpu.make_async_copy(others, others, g_send).wait()
    pltpu.make_async_copy(others_s, others_s, s_send).wait()


def solution(mesh):
    DP, MP = mesh.shape["dp"], mesh.shape["mp"]
    N = DP * MP

    def body(q_new, k_new, v_new, k_cache, v_cache, lengths, memory, norm_z, beta, out_weight, residual_in, final_gain, embedding):
        B, H, L, HD = k_cache.shape
        FW = out_weight.shape[1]
        V, D = embedding.shape
        C = FW // LANES
        CP = up(C, 16 // math.gcd(B, 16))
        pairs, PP = B * H, up(B * H, 8)
        S = DP * B
        dma = pltpu.SemaphoreType.DMA
        anywhere = pl.BlockSpec(memory_space=pl.ANY)
        vmem = pl.BlockSpec(memory_space=pltpu.VMEM)
        hidden, log_probs = pl.pallas_call(
            functools.partial(kernel, DP, MP, B, H, HD, L, FW, CP),
            out_shape=(pltpu.VMEM((B, FW), BF16), pltpu.VMEM((S, V), F32)),
            in_specs=[anywhere] * 13,
            out_specs=(vmem, vmem),
            scratch_shapes=[
                pltpu.VMEM((B, H, HD), BF16),
                pltpu.VMEM((B, H, HD), BF16),
                pltpu.VMEM((B, H, HD), BF16),
                pltpu.VMEM((B, H, HD), F32),
                pltpu.VMEM((B, FW), BF16),
                pltpu.VMEM((1, D), F32),
                pltpu.VMEM((pairs, L, HD), BF16),
                pltpu.VMEM((pairs, L, HD), BF16),
                pltpu.VMEM((pairs, HD, HD), F32),
                pltpu.VMEM(out_weight.shape, BF16),
                pltpu.VMEM((V, D), BF16),
                pltpu.SMEM(lengths.shape, jnp.int32),
                pltpu.SMEM(beta.shape, F32),
                pltpu.VMEM((4, PP, HD), F32),
                pltpu.VMEM((MP, PP, HD), BF16),
                pltpu.VMEM((B * CP, LANES), F32),
                pltpu.VMEM((N, B * CP, LANES), BF16),
                pltpu.VMEM((MP, DP * B * CP, LANES), F32),
                pltpu.VMEM((DP * MP, 1, up(S, LANES)), F32),
                pltpu.VMEM((MP, 1, up(S, LANES)), F32),
                dma((8,)),
                dma((pairs,)),
                dma((pairs,)),
                dma((pairs,)),
                dma((MP,)),
                dma,
                dma((MP,)),
                dma((MP,)),
                dma,
                dma,
                dma,
                dma,
                dma((MP,)),
                dma((MP,)),
                dma((MP,)),
                dma((MP,)),
            ],
            compiler_params=pltpu.CompilerParams(collective_id=0, has_side_effects=True),
            name="decode_step",
        )(
            lengths, beta, q_new, k_new, v_new, k_cache, v_cache, memory, norm_z, out_weight, residual_in,
            final_gain.reshape(1, D), embedding,
        )
        return hidden, log_probs

    in_specs = (
        P("dp", "mp", None),
        P("dp", "mp", None),
        P("dp", "mp", None),
        P("dp", "mp", None, None),
        P("dp", "mp", None, None),
        P("dp"),
        P("dp", "mp", None, None),
        P("dp", "mp", None),
        P("mp"),
        P(None, "mp"),
        P("dp", "mp"),
        P(),
        P(("dp", "mp"), None),
    )
    out_specs = (P("dp", "mp"), P(None, ("dp", "mp")))
    return jax.shard_map(body, mesh=mesh, in_specs=in_specs, out_specs=out_specs, check_vma=False)
```
